8 devices in a mesh: data: 8 (over z, y, x, core).
Axes of the slice: x: 2, y: 2, z: 1, core: 2. Of those that a mesh axis runs over, the one named last changes fastest.
Arguments:
- x_tokens: bfloat16 [4096, 384], P('data')
- labels: int32 [3, 4096], P(None, 'data')
- w_up: bfloat16 [4, 384, 1536], replicated
- w_down: bfloat16 [4, 1536, 384], replicated
- task_heads: bfloat16 [3, 384, 13], replicated
Outputs:
- output 1: float32 [3], replicated
- output 2: float32 [3, 3], replicated
- output 3: float32 [4, 589824], P(None, 'data')
- output 4: float32 [4, 589824], P(None, 'data')
All inputs are finite; a program needn't handle non-finite values.
Results may differ from the reference program's by a relative error of at most 0.00354996.
Values are sent between devices in bfloat16 or wider.
A program may use at most 1 GiB of HBM per device.

```python
import jax
import jax.numpy as jnp
from jax import lax

D_MODEL = 384
D_FF = 1536
NUM_TASKS = 3
NUM_CLASSES = 13
NUM_LAYERS = 4
TOK_DEV = 512
NUM_DEV = 8
EG_STEPS = 20


def setup_inputs(seed: int = 0) -> dict:
    base_key = jax.random.key(seed)
    sub_keys = jax.random.split(base_key, 10)
    num_tokens = NUM_DEV * TOK_DEV
    x_tokens = jax.random.normal(sub_keys[0], (num_tokens, D_MODEL), jnp.float32).astype(jnp.bfloat16)
    w_up = (jax.random.normal(sub_keys[1], (NUM_LAYERS, D_MODEL, D_FF), jnp.float32) * D_MODEL ** -0.5).astype(jnp.bfloat16)
    w_down = (jax.random.normal(sub_keys[2], (NUM_LAYERS, D_FF, D_MODEL), jnp.float32) * D_FF ** -0.5).astype(jnp.bfloat16)
    shared_head = jax.random.normal(sub_keys[3], (D_MODEL, NUM_CLASSES), jnp.float32)
    head_noise = jax.random.normal(sub_keys[4], (NUM_TASKS, D_MODEL, NUM_CLASSES), jnp.float32)
    task_order = jax.random.permutation(sub_keys[5], NUM_TASKS)
    task_sign = jnp.where(task_order < NUM_TASKS // 2, -1.0, 1.0)
    task_heads = ((task_sign[:, None, None] * shared_head[None] + 0.6 * head_noise) * D_MODEL ** -0.5).astype(jnp.bfloat16)
    dev_shift = jax.random.randint(sub_keys[6], (NUM_DEV, 1), 0, NUM_CLASSES)
    local_lab = jax.random.randint(sub_keys[7], (NUM_DEV, TOK_DEV), 0, max(NUM_CLASSES // 2, 1))
    base_lab = ((local_lab + dev_shift) % NUM_CLASSES).reshape(1, num_tokens)
    free_lab = jax.random.randint(sub_keys[8], (NUM_TASKS, num_tokens), 0, NUM_CLASSES)
    free_pick = jax.random.randint(sub_keys[9], (NUM_TASKS, num_tokens), 0, 4)
    labels = jnp.where(free_pick == 0, free_lab, base_lab).astype(jnp.int32)
    return {'x_tokens': x_tokens, 'labels': labels, 'w_up': w_up, 'w_down': w_down, 'task_heads': task_heads}


def simplex_weights(gram_mat):
    temperature = jnp.trace(gram_mat) / NUM_TASKS
    alpha_vec = jnp.full((NUM_TASKS,), 1.0 / NUM_TASKS, jnp.float32)
    for step_idx in range(EG_STEPS):
        grad_pull = jnp.sum(gram_mat * alpha_vec[None, :], axis=1)
        alpha_vec = alpha_vec * jnp.exp(-grad_pull / temperature)
        alpha_vec = alpha_vec / jnp.sum(alpha_vec)
    return alpha_vec


def block_grads(x_block, lab_block, w_up, w_down, task_heads):
    hidden = x_block
    saved_acts = []
    for layer_idx in range(NUM_LAYERS):
        pre_act = jnp.dot(hidden, w_up[layer_idx], preferred_element_type=jnp.float32)
        act_val, gelu_slope = jax.jvp(jax.nn.gelu, (pre_act,), (jnp.ones_like(pre_act),))
        act_bf = act_val.astype(jnp.bfloat16)
        mlp_out = jnp.dot(act_bf, w_down[layer_idx], preferred_element_type=jnp.float32)
        saved_acts.append((hidden, act_bf, gelu_slope))
        hidden = (hidden.astype(jnp.float32) + mlp_out).astype(jnp.bfloat16)
    heads_f = task_heads.astype(jnp.float32)
    logits = jnp.einsum('bd,tdc->tbc', hidden.astype(jnp.float32), heads_f)
    soft_probs = jax.nn.softmax(logits, axis=-1)
    onehot = (lab_block[:, :, None] == jnp.arange(NUM_CLASSES)[None, None, :]).astype(jnp.float32)
    head_err = (soft_probs - onehot).astype(jnp.bfloat16)
    d_hidden = jnp.einsum('tbc,tdc->tbd', head_err.astype(jnp.float32), heads_f).astype(jnp.bfloat16)
    up_list = []
    down_list = []
    for layer_idx in range(NUM_LAYERS - 1, -1, -1):
        hidden_in, act_bf, gelu_slope = saved_acts[layer_idx]
        d_hid_f = d_hidden.astype(jnp.float32)
        down_list.append(jnp.einsum('bf,tbd->tfd', act_bf.astype(jnp.float32), d_hid_f))
        d_act = jnp.einsum('tbd,fd->tbf', d_hid_f, w_down[layer_idx].astype(jnp.float32))
        d_pre = (d_act * gelu_slope[None]).astype(jnp.bfloat16)
        d_pre_f = d_pre.astype(jnp.float32)
        up_list.append(jnp.einsum('bd,tbf->tdf', hidden_in.astype(jnp.float32), d_pre_f))
        if layer_idx > 0:
            d_hidden = (d_hid_f + jnp.einsum('tbf,df->tbd', d_pre_f, w_up[layer_idx].astype(jnp.float32))).astype(jnp.bfloat16)
    return jnp.stack(up_list[::-1]), jnp.stack(down_list[::-1])


def reference(x_tokens, labels, w_up, w_down, task_heads):
    x_blocks = x_tokens.reshape(NUM_DEV, TOK_DEV, D_MODEL)
    lab_blocks = jnp.transpose(labels.reshape(NUM_TASKS, NUM_DEV, TOK_DEV), (1, 0, 2))
    zero_up = jnp.zeros((NUM_LAYERS, NUM_TASKS, D_MODEL, D_FF), jnp.float32)
    zero_down = jnp.zeros((NUM_LAYERS, NUM_TASKS, D_FF, D_MODEL), jnp.float32)

    def scan_body(running, token_block):
        up_grads, down_grads = block_grads(token_block[0], token_block[1], w_up, w_down, task_heads)
        return (running[0] + up_grads, running[1] + down_grads), None

    totals, unused = lax.scan(scan_body, (zero_up, zero_down), (x_blocks, lab_blocks))
    inv_tokens = 1.0 / (NUM_DEV * TOK_DEV)
    flat_up = (totals[0] * inv_tokens).reshape(NUM_LAYERS, NUM_TASKS, D_MODEL * D_FF)
    flat_down = (totals[1] * inv_tokens).reshape(NUM_LAYERS, NUM_TASKS, D_FF * D_MODEL)
    gram_mat = jnp.einsum('lts,lus->tu', flat_up, flat_up) + jnp.einsum('lts,lus->tu', flat_down, flat_down)
    task_weights = simplex_weights(gram_mat)
    grad_up = jnp.einsum('t,lts->ls', task_weights, flat_up)
    grad_down = jnp.einsum('t,lts->ls', task_weights, flat_down)
    return (task_weights, gram_mat, grad_up, grad_down)
```

```python
import math

import jax
import jax.numpy as jnp
from jax import lax
from jax.experimental import pallas as pl
from jax.experimental.pallas import tpu as pltpu
from jax.sharding import PartitionSpec as P

EG_STEPS = 20
MESH = pl.DeviceIdType.MESH
GELU_C = math.sqrt(2.0 / math.pi)
GELU_A = 0.044715
F32 = jnp.float32
BF16 = jnp.bfloat16
PAIRS = ((0, 0), (0, 1), (0, 2), (1, 1), (1, 2), (2, 2))
CORES = 2
CHIPS = 4


def dot_nn(lhs, rhs):
    return lax.dot_general(lhs, rhs, (((1,), (0,)), ((), ())), preferred_element_type=F32)


def dot_nt(lhs, rhs):
    return lax.dot_general(lhs, rhs, (((1,), (1,)), ((), ())), preferred_element_type=F32)


def dot_tn(lhs, rhs):
    return lax.dot_general(lhs, rhs, (((0,), (0,)), ((), ())), preferred_element_type=F32)


def dot_tt(lhs, rhs):
    return lax.dot_general(lhs, rhs, (((0,), (1,)), ((), ())), preferred_element_type=F32)


def gelu_act(pre):
    tanh_val = jnp.tanh(pre * (GELU_C + (GELU_C * GELU_A) * (pre * pre)))
    return pre * (0.5 * tanh_val + 0.5)


def gelu_slope(pre):
    sq_pre = pre * pre
    tanh_val = jnp.tanh(pre * (GELU_C + (GELU_C * GELU_A) * sq_pre))
    rise = pre * (0.5 * GELU_C + (1.5 * GELU_C * GELU_A) * sq_pre)
    return (0.5 * tanh_val + 0.5) + rise * (1.0 - tanh_val * tanh_val)


def trunk_kernel(inv_tokens, x_ref, lab_ref, w1_hbm, w2_hbm, head_ref, stat_ref, outu_ref, outd_ref,
                 w1, w2, xg, lg, hs, pre, act, akeep, dstack, dcat, sbuf, scat, accu, accd, recvu, recvd,
                 gsend, grecv, mtile, w_sem, xs_sem, xr_sem, ls_sem, lr_sem, us_sem, ur_sem, ds_sem, dr_sem,
                 ms_sem, mr_sem, gs_sem, gr_sem):
    num_layers, num_tasks = w1.shape[0], head_ref.shape[0]
    tok, dim = x_ref.shape
    ff = w1.shape[2]
    ffq = ff // CHIPS
    num_dev = CORES * CHIPS
    me = lax.axis_index('data')
    chip, core = me // CORES, me % CORES
    mate = me + 1 - 2 * core
    mcore = 1 - core
    cx, cy = chip % 2, chip // 2
    peer_chip = (cy * 2 + (1 - cx), (1 - cy) * 2 + cx, (1 - cy) * 2 + (1 - cx))
    peers = tuple(pc * CORES + core for pc in peer_chip)

    w_copies = []
    for layer in range(num_layers):
        c1 = pltpu.make_async_copy(w1_hbm.at[layer], w1.at[layer], w_sem.at[0, layer])
        c2 = pltpu.make_async_copy(w2_hbm.at[layer], w2.at[layer], w_sem.at[1, layer])
        c1.start()
        c2.start()
        w_copies.append((c1, c2))

    barrier = pltpu.get_barrier_semaphore()
    for step in range(1, num_dev):
        pl.semaphore_signal(barrier, inc=1, device_id=(lax.rem(me + step, num_dev),), device_id_type=MESH)
    pl.semaphore_wait(barrier, num_dev - 1)

    x_copies, l_copies = [], []
    for slot in range(3):
        x_copies.append(pltpu.make_async_remote_copy(
            src_ref=x_ref, dst_ref=xg.at[slot], send_sem=xs_sem.at[slot], recv_sem=xr_sem.at[slot],
            device_id=(peers[slot],), device_id_type=MESH))
        l_copies.append(pltpu.make_async_remote_copy(
            src_ref=lab_ref, dst_ref=lg.at[slot], send_sem=ls_sem.at[slot], recv_sem=lr_sem.at[slot],
            device_id=(peers[slot],), device_id_type=MESH))
    for slot in range(3):
        x_copies[slot].start()
        l_copies[slot].start()

    fk = pl.ds(pl.multiple_of(chip * ffq, 128), ffq)

    def forward(layer):
        h_in = hs[layer]

        @pl.loop(0, 3)
        def _(blk):
            cols = pl.ds(pl.multiple_of(blk * 512, 512), 512)
            p_val = dot_nn(h_in, w1[layer, :, cols])
            pre[layer, :, cols] = p_val
            act[:, cols] = gelu_act(p_val).astype(BF16)

        akeep[layer] = act[:, fk]
        hs[layer + 1] = (h_in.astype(F32) + dot_nn(act[...], w2[layer])).astype(BF16)

    def weight_grads(layer, first):
        down = dot_tn(akeep[layer], dcat[...])
        up = dot_tn(hs[layer], scat[...])
        for task in range(num_tasks):
            d_new = down[:, task * dim:(task + 1) * dim].reshape(2, ffq // 2, dim)
            u_new = up[:, task * ffq:(task + 1) * ffq].reshape(CHIPS, CORES, dim // 8, ffq)

            if first:
                accd[layer, task] = d_new
                accu[layer, task] = u_new
            else:
                accd[layer, task] += d_new
                accu[layer, task] += u_new

    def backward_full(layer, first):
        @pl.loop(0, 3)
        def _(blk):
            cols = pl.ds(pl.multiple_of(blk * 512, 512), 512)
            slope = gelu_slope(pre[layer, :, cols])
            w_blk = w2[layer, cols, :]
            for task in range(num_tasks):
                d_act = dot_nt(dstack[task], w_blk)
                sbuf[task, :, cols] = (d_act * slope).astype(BF16)

        for task in range(num_tasks):
            scat[:, task * ffq:(task + 1) * ffq] = sbuf[task, :, fk]
        weight_grads(layer, first)
        for task in range(num_tasks):
            d_new = dstack[task].astype(F32) + dot_nt(sbuf[task], w1[layer])
            d_new = d_new.astype(BF16)
            dstack[task] = d_new
            dcat[:, task * dim:(task + 1) * dim] = d_new

    def backward_first(first):
        slope = gelu_slope(pre[0, :, fk])
        for task in range(num_tasks):
            d_act = dot_nt(dstack[task], w2[0, fk, :])
            scat[:, task * ffq:(task + 1) * ffq] = (d_act * slope).astype(BF16)
        weight_grads(0, first)

    def head_errors(labels):
        z_val = hs[num_layers]
        for task in range(num_tasks):
            logits = dot_tt(head_ref[task], z_val)
            shifted = jnp.exp(logits - jnp.max(logits, axis=0, keepdims=True))
            probs = shifted / jnp.sum(shifted, axis=0, keepdims=True)
            rows = lax.broadcasted_iota(jnp.int32, probs.shape, 0)
            onehot = (rows == labels[task:task + 1, :]).astype(F32)
            err = (probs - onehot).astype(BF16)
            d_val = dot_tt(err, head_ref[task]).astype(BF16)
            dstack[task] = d_val
            dcat[:, task * dim:(task + 1) * dim] = d_val

    u_copies, d_copies = [], []
    for layer in range(num_layers):
        u_copies.append(pltpu.make_async_remote_copy(
            src_ref=accu.at[layer, :, :, mcore], dst_ref=recvu.at[layer], send_sem=us_sem.at[layer],
            recv_sem=ur_sem.at[layer], device_id=(mate,), device_id_type=MESH))
        d_copies.append(pltpu.make_async_remote_copy(
            src_ref=accd.at[layer, :, mcore], dst_ref=recvd.at[layer], send_sem=ds_sem.at[layer],
            recv_sem=dr_sem.at[layer], device_id=(mate,), device_id_type=MESH))

    def zero_acc(layer):
        accu[layer] = jnp.zeros(accu.shape[1:], F32)
        accd[layer] = jnp.zeros(accd.shape[1:], F32)

    @pl.loop(0, num_layers)
    def _(layer):
        zero_acc(layer)

    @pl.loop(0, CHIPS)
    def _(quarter):
        @pl.when(quarter == 0)
        def _():
            hs[0] = x_ref[...]

        for slot in range(3):
            @pl.when(quarter == slot + 1)
            def _():
                x_copies[slot].wait_recv()
                l_copies[slot].wait_recv()
                hs[0] = xg[slot]

        for layer in range(num_layers):
            @pl.when(quarter == 0)
            def _():
                w_copies[layer][0].wait()
                w_copies[layer][1].wait()

        @pl.loop(0, num_layers)
        def _(layer):
            forward(layer)

        @pl.when(quarter == 0)
        def _():
            head_errors(lab_ref[...])

        @pl.when(quarter > 0)
        def _():
            head_errors(lg[jnp.maximum(quarter - 1, 0)])

        @pl.loop(0, num_layers - 1)
        def _(back):
            layer = num_layers - 1 - back
            backward_full(layer, False)
            for sent in range(1, num_layers):
                @pl.when(jnp.logical_and(quarter == CHIPS - 1, layer == sent))
                def _():
                    u_copies[sent].start()
                    d_copies[sent].start()

        backward_first(False)

    u_copies[0].start()
    d_copies[0].start()
    for slot in range(3):
        x_copies[slot].wait_send()
        l_copies[slot].wait_send()

    sums = tuple(jnp.zeros((8, 128), F32) for _ in PAIRS)

    def fold(val):
        tiles = val.reshape(-1, 8, val.shape[-1])
        part = jnp.sum(tiles, axis=0)
        out = part[:, :128]
        for piece in range(1, part.shape[-1] // 128):
            out = out + part[:, piece * 128:(piece + 1) * 128]
        return out

    def gram(sums, grads):
        return tuple(acc + fold(grads[t] * grads[s]) for acc, (t, s) in zip(sums, PAIRS))

    for layer in range(num_layers - 1, -1, -1):
        u_copies[layer].wait_recv()
        d_copies[layer].wait_recv()

        @pl.loop(0, CHIPS, init_carry=sums)
        def sums(block, carry):
            grads = []
            for task in range(num_tasks):
                val = (accu[layer, task, block, core] + recvu[layer, task, block]) * inv_tokens
                recvu[layer, task, block] = val
                grads.append(val)
            return gram(carry, grads)

        @pl.loop(0, 4, init_carry=sums)
        def sums(block, carry):
            rows = pl.ds(pl.multiple_of(block * 48, 48), 48)
            grads = []
            for task in range(num_tasks):
                val = (accd[layer, task, core, rows] + recvd[layer, task, rows]) * inv_tokens
                recvd[layer, task, rows] = val
                grads.append(val)
            return gram(carry, grads)

    tile_rows = lax.broadcasted_iota(jnp.int32, (8, 128), 0)
    my_tile = jnp.zeros((8, 128), F32)
    for row, acc in enumerate(sums):
        my_tile = jnp.where(tile_rows == row, jnp.sum(acc, axis=0, keepdims=True), my_tile)
    mtile[me] = my_tile
    m_copies = []
    for step in range(1, num_dev):
        m_copies.append(pltpu.make_async_remote_copy(
            src_ref=mtile.at[me], dst_ref=mtile.at[me], send_sem=ms_sem.at[step - 1], recv_sem=mr_sem.at[step - 1],
            device_id=(lax.rem(me + step, num_dev),), device_id_type=MESH))
    for copy in m_copies:
        copy.start()
    for layer in range(num_layers):
        u_copies[layer].wait_send()
        d_copies[layer].wait_send()
    for step in range(1, num_dev):
        src_dev = lax.rem(me + num_dev - step, num_dev)
        pltpu.make_async_remote_copy(
            src_ref=mtile.at[src_dev], dst_ref=mtile.at[src_dev], send_sem=ms_sem.at[step - 1],
            recv_sem=mr_sem.at[step - 1], device_id=(lax.rem(me + step, num_dev),), device_id_type=MESH).wait_recv()
    total = mtile[0]
    for dev in range(1, num_dev):
        total = total + mtile[dev]
    total = jnp.broadcast_to(jnp.sum(total, axis=1, keepdims=True), (8, 128))
    entry = {}
    for row, (t, s) in enumerate(PAIRS):
        val = jnp.broadcast_to(total[row:row + 1, :], (8, 128))
        entry[t, s] = val
        entry[s, t] = val
    tau = (entry[0, 0] + entry[1, 1] + entry[2, 2]) / num_tasks
    alpha = [jnp.full((8, 128), 1.0 / num_tasks, F32) for _ in range(num_tasks)]
    for step in range(EG_STEPS):
        pulls = [entry[t, 0] * alpha[0] + entry[t, 1] * alpha[1] + entry[t, 2] * alpha[2] for t in range(num_tasks)]
        alpha = [alpha[t] * jnp.exp(-pulls[t] / tau) for t in range(num_tasks)]
        norm = alpha[0] + alpha[1] + alpha[2]
        alpha = [a / norm for a in alpha]
    lanes = lax.broadcasted_iota(jnp.int32, (8, 128), 1)
    stat = jnp.zeros((8, 128), F32)
    for t in range(num_tasks):
        stat = jnp.where(jnp.logical_and(tile_rows == 0, lanes == t), alpha[t], stat)
        for s in range(num_tasks):
            stat = jnp.where(jnp.logical_and(tile_rows == 1 + t, lanes == s), entry[t, s], stat)
    stat_ref[...] = stat

    wts = [a[0:1, 0:1] for a in alpha]

    for block in range(CHIPS):
        for layer in range(num_layers):
            gsend[block, layer] = (wts[0] * recvu[layer, 0, block] + wts[1] * recvu[layer, 1, block]
                                   + wts[2] * recvu[layer, 2, block])
    g_copies = []
    for slot in range(3):
        g_copies.append(pltpu.make_async_remote_copy(
            src_ref=gsend.at[peer_chip[slot]], dst_ref=grecv.at[slot], send_sem=gs_sem.at[slot],
            recv_sem=gr_sem.at[slot], device_id=(peers[slot],), device_id_type=MESH))
        g_copies[-1].start()

    def put_rows(out_ref, layer, rows, row0, row_tiles, col_tile, val):
        for piece in range(val.shape[1] // 128):
            start = row0 * row_tiles * num_layers + (col_tile + piece) * num_layers + layer
            out_ref[pl.ds(start, rows, stride=row_tiles * num_layers), :] = val[:, piece * 128:(piece + 1) * 128]

    @pl.loop(0, 4)
    def _(block):
        rows = pl.ds(pl.multiple_of(block * 48, 48), 48)
        for layer in range(num_layers):
            val = wts[0] * recvd[layer, 0, rows] + wts[1] * recvd[layer, 1, rows] + wts[2] * recvd[layer, 2, rows]
            put_rows(outd_ref, layer, 48, block * 48, dim // 128, 0, val)

    for layer in range(num_layers):
        put_rows(outu_ref, layer, 48, 0, ff // 128, chip * (ffq // 128), gsend[chip, layer])
    for slot in range(3):
        g_copies[slot].wait_recv()
        for layer in range(num_layers):
            put_rows(outu_ref, layer, 48, 0, ff // 128, peer_chip[slot] * (ffq // 128), grecv[slot, layer])
    for slot in range(3):
        g_copies[slot].wait_send()
    for copy in m_copies:
        copy.wait_send()


def solution(mesh):
    num_dev = mesh.shape['data']

    def local_step(x_local, lab_local, w_up, w_down, task_heads):
        num_layers, dim, ff = w_up.shape
        num_tasks = task_heads.shape[0]
        tok = x_local.shape[0]
        ffq = ff // CHIPS
        inv_tokens = 1.0 / (tok * num_dev)
        share = num_layers * dim * ff // num_dev // 128
        vmem = pl.BlockSpec(memory_space=pltpu.VMEM)
        hbm = pl.BlockSpec(memory_space=pl.ANY)

        def body(*refs):
            trunk_kernel(inv_tokens, *refs)

        dma = pltpu.SemaphoreType.DMA
        stat, out_up, out_down = pl.pallas_call(
            body,
            out_shape=(jax.ShapeDtypeStruct((8, 128), F32), jax.ShapeDtypeStruct((share, 128), F32),
                       jax.ShapeDtypeStruct((share, 128), F32)),
            in_specs=[vmem, vmem, hbm, hbm, vmem],
            out_specs=(vmem, vmem, vmem),
            scratch_shapes=[
                pltpu.VMEM((num_layers, dim, ff), BF16),
                pltpu.VMEM((num_layers, ff, dim), BF16),
                pltpu.VMEM((3, tok, dim), BF16),
                pltpu.VMEM((3, num_tasks, tok), jnp.int32),
                pltpu.VMEM((num_layers + 1, tok, dim), BF16),
                pltpu.VMEM((num_layers, tok, ff), F32),
                pltpu.VMEM((tok, ff), BF16),
                pltpu.VMEM((num_layers, tok, ffq), BF16),
                pltpu.VMEM((num_tasks, tok, dim), BF16),
                pltpu.VMEM((tok, num_tasks * dim), BF16),
                pltpu.VMEM((num_tasks, tok, ff), BF16),
                pltpu.VMEM((tok, num_tasks * ffq), BF16),
                pltpu.VMEM((num_layers, num_tasks, CHIPS, CORES, dim // num_dev, ffq), F32),
                pltpu.VMEM((num_layers, num_tasks, CORES, ffq // CORES, dim), F32),
                pltpu.VMEM((num_layers, num_tasks, CHIPS, dim // num_dev, ffq), F32),
                pltpu.VMEM((num_layers, num_tasks, ffq // CORES, dim), F32),
                pltpu.VMEM((CHIPS, num_layers, dim // num_dev, ffq), F32),
                pltpu.VMEM((3, num_layers, dim // num_dev, ffq), F32),
                pltpu.VMEM((num_dev, 8, 128), F32),
                dma((2, num_layers)), dma((3,)), dma((3,)), dma((3,)), dma((3,)),
                dma((num_layers,)), dma((num_layers,)), dma((num_layers,)), dma((num_layers,)),
                dma((num_dev - 1,)), dma((num_dev - 1,)), dma((3,)), dma((3,)),
            ],
            compiler_params=pltpu.CompilerParams(
                collective_id=0, has_side_effects=True, vmem_limit_bytes=67043328),
        )(x_local, lab_local, w_up, w_down, task_heads)

        def unpack(packed):
            tiles = packed.reshape(share // num_layers, num_layers, 128)
            return jnp.transpose(tiles, (1, 0, 2)).reshape(num_layers, -1)

        return stat[0, :num_tasks], stat[1:1 + num_tasks, :num_tasks], unpack(out_up), unpack(out_down)

    return jax.shard_map(local_step, mesh=mesh, in_specs=(P('data', None), P(None, 'data'), P(), P(), P()),
                         out_specs=(P(), P(), P(None, 'data'), P(None, 'data')), check_vma=False)
```

```python
import math

import jax
import jax.numpy as jnp
from jax import lax
from jax.experimental import pallas as pl
from jax.experimental.pallas import tpu as pltpu
from jax.sharding import PartitionSpec as P

EG_STEPS = 20
MESH = pl.DeviceIdType.MESH
GELU_C = math.sqrt(2.0 / math.pi)
GELU_A = 0.044715
F32 = jnp.float32
BF16 = jnp.bfloat16
PAIRS = ((0, 0), (0, 1), (0, 2), (1, 1), (1, 2), (2, 2))
CORES = 2
CHIPS = 4
UNROLL = True


def dot_nn(lhs, rhs):
    return lax.dot_general(lhs, rhs, (((1,), (0,)), ((), ())), preferred_element_type=F32)


def dot_nt(lhs, rhs):
    return lax.dot_general(lhs, rhs, (((1,), (1,)), ((), ())), preferred_element_type=F32)


def dot_tn(lhs, rhs):
    return lax.dot_general(lhs, rhs, (((0,), (0,)), ((), ())), preferred_element_type=F32)


def dot_tt(lhs, rhs):
    return lax.dot_general(lhs, rhs, (((0,), (1,)), ((), ())), preferred_element_type=F32)


def gelu_act(pre):
    tanh_val = jnp.tanh(pre * (GELU_C + (GELU_C * GELU_A) * (pre * pre)))
    return pre * (0.5 * tanh_val + 0.5)


def gelu_slope(pre):
    sq_pre = pre * pre
    tanh_val = jnp.tanh(pre * (GELU_C + (GELU_C * GELU_A) * sq_pre))
    rise = pre * (0.5 * GELU_C + (1.5 * GELU_C * GELU_A) * sq_pre)
    return (0.5 * tanh_val + 0.5) + rise * (1.0 - tanh_val * tanh_val)


def trunk_kernel(inv_tokens, x_ref, lab_ref, w1_hbm, w2_hbm, head_ref, stat_ref, outu_ref, outd_ref,
                 w1, w2, xg, lg, hs, pre, akeep, afk, dcat, dsend, drecv, sbuf, scat, acc, mtile,
                 w_sem, xs_sem, xr_sem, ls_sem, lr_sem, es_sem, er_sem, ps_sem, pr_sem,
                 ms_sem, mr_sem, gs_sem, gr_sem, free_sem):
    num_layers, num_tasks = w1.shape[0], head_ref.shape[0]
    tok, dim = x_ref.shape
    ff = w1.shape[2]
    ffq = ff // CHIPS
    half = dim // CORES
    rows48 = dim // (CORES * CHIPS)
    num_dev = CORES * CHIPS
    me = lax.axis_index('data')
    chip, core = me // CORES, me % CORES
    mate = me + 1 - 2 * core
    mcore = 1 - core
    cx, cy = chip % 2, chip // 2
    peer_chip = (cy * 2 + (1 - cx), (1 - cy) * 2 + cx, (1 - cy) * 2 + (1 - cx))
    peers = tuple(pc * CORES + core for pc in peer_chip)

    w_copies = []
    for layer in range(num_layers):
        c1 = pltpu.make_async_copy(w1_hbm.at[layer], w1.at[layer], w_sem.at[0, layer])
        c2 = pltpu.make_async_copy(w2_hbm.at[layer], w2.at[layer], w_sem.at[1, layer])
        c1.start()
        c2.start()
        w_copies.append((c1, c2))

    barrier = pltpu.get_barrier_semaphore()
    for step in range(1, num_dev):
        pl.semaphore_signal(barrier, inc=1, device_id=(lax.rem(me + step, num_dev),), device_id_type=MESH)
    pl.semaphore_wait(barrier, num_dev - 1)

    def remote(src, dst, send, recv, dev):
        return pltpu.make_async_remote_copy(src_ref=src, dst_ref=dst, send_sem=send, recv_sem=recv,
                                            device_id=(dev,), device_id_type=MESH)

    x_copies = [remote(x_ref, xg.at[s], xs_sem.at[s], xr_sem.at[s], peers[s]) for s in range(3)]
    l_copies = [remote(lab_ref, lg.at[s], ls_sem.at[s], lr_sem.at[s], peers[s]) for s in range(3)]
    e_copies = [[remote(dsend.at[v], drecv.at[s, v], es_sem.at[s, v], er_sem.at[s, v], peers[s])
                 for v in range(num_layers - 1)] for s in range(2)]
    p_copies = [remote(acc.at[v, :, mcore], pre.at[pl.ds(v * num_tasks, num_tasks), pl.ds(0, dim)],
                       ps_sem.at[v], pr_sem.at[v], mate) for v in range(num_layers)]
    for slot in (2, 0, 1):
        x_copies[slot].start()
        l_copies[slot].start()

    fk = pl.ds(pl.multiple_of(chip * ffq, 128), ffq)

    def wide_blocks(body):
        if UNROLL:
            for blk in range(2):
                body(blk)
        else:
            @pl.loop(0, 2)
            def _(blk):
                body(blk)

    def wide_cols(blk):
        return pl.ds(pl.multiple_of(blk * 2 * ffq, 128), 2 * ffq)

    def forward(layer, keep):
        h_in = hs[layer]

        def body(blk):
            p_val = dot_nn(h_in, w1[layer, :, wide_cols(blk)])
            if keep:
                pre[(layer - 1) * CHIPS + 2 * blk] = p_val[:, :ffq]
                pre[(layer - 1) * CHIPS + 2 * blk + 1] = p_val[:, ffq:]
            sbuf[0, :, wide_cols(blk)] = gelu_act(p_val).astype(BF16)

        wide_blocks(body)
        if keep:
            akeep[layer - 1] = sbuf[0, :, fk]
        hs[layer + 1] = (h_in.astype(F32) + dot_nn(sbuf[0], w2[layer])).astype(BF16)

    def add_down(layer, a_val, d_val):
        down = dot_tn(a_val, d_val)
        for task in range(num_tasks):
            for par in range(CORES):
                acc[layer, task, par, half:] += down[par * half:(par + 1) * half, task * dim:(task + 1) * dim]

    def add_up(layer, h_val):
        up = dot_tn(h_val, scat[...])
        for task in range(num_tasks):
            for par in range(CORES):
                for blk in range(CHIPS):
                    row = (blk * CORES + par) * rows48
                    acc[layer, task, par, blk * rows48:(blk + 1) * rows48] += (
                        up[row:row + rows48, task * ffq:(task + 1) * ffq])

    def backward_full(layer):
        def body(blk):
            w_blk = w2[layer, wide_cols(blk), :]
            slopes = [gelu_slope(pre[(layer - 1) * CHIPS + 2 * blk + i]) for i in range(2)]
            for task in range(num_tasks):
                d_act = dot_nt(dcat[:, task * dim:(task + 1) * dim], w_blk)
                for i in range(2):
                    cols = pl.ds(pl.multiple_of((2 * blk + i) * ffq, 128), ffq)
                    sbuf[task, :, cols] = (d_act[:, i * ffq:(i + 1) * ffq] * slopes[i]).astype(BF16)

        wide_blocks(body)
        for task in range(num_tasks):
            scat[:, task * ffq:(task + 1) * ffq] = sbuf[task, :, fk]
        add_down(layer, akeep[layer - 1], dcat[...])
        for task in range(num_tasks):
            cols = slice(task * dim, (task + 1) * dim)
            dcat[:, cols] = (dcat[:, cols].astype(F32) + dot_nt(sbuf[task], w1[layer])).astype(BF16)
        add_up(layer, hs[layer])

    def backward_part(layer, h_val, d_ref):
        p_val = dot_nn(h_val, w1[layer, :, fk])
        slope = gelu_slope(p_val)
        afk[...] = gelu_act(p_val).astype(BF16)
        for task in range(num_tasks):
            d_act = dot_nt(d_ref[:, task * dim:(task + 1) * dim], w2[layer, fk, :])
            scat[:, task * ffq:(task + 1) * ffq] = (d_act * slope).astype(BF16)
        add_down(layer, afk[...], d_ref[...])
        add_up(layer, h_val)

    def head_errors(labels):
        z_val = hs[num_layers]
        for task in range(num_tasks):
            logits = dot_nt(head_ref[task], z_val)
            shifted = jnp.exp(logits - jnp.max(logits, axis=0, keepdims=True))
            probs = shifted / jnp.sum(shifted, axis=0, keepdims=True)
            rows = lax.broadcasted_iota(jnp.int32, probs.shape, 0)
            onehot = (rows == labels[task:task + 1, :]).astype(F32)
            err = (probs - onehot).astype(BF16)
            dcat[:, task * dim:(task + 1) * dim] = dot_tn(err, head_ref[task]).astype(BF16)

    @pl.loop(0, num_layers)
    def _(layer):
        acc[layer] = jnp.zeros(acc.shape[1:], F32)

    @pl.loop(0, 2)
    def _(turn):
        @pl.when(turn == 0)
        def _():
            hs[0] = x_ref[...]
            w_copies[0][0].wait()
            w_copies[0][1].wait()

        @pl.when(turn == 1)
        def _():
            x_copies[2].wait_recv()
            l_copies[2].wait_recv()
            hs[0] = xg[2]

        forward(0, False)

        @pl.loop(1, num_layers)
        def _(layer):
            for late in range(1, num_layers):
                @pl.when(jnp.logical_and(turn == 0, layer == late))
                def _():
                    w_copies[late][0].wait()
                    w_copies[late][1].wait()
            forward(layer, True)

        @pl.when(turn == 0)
        def _():
            head_errors(lab_ref[...])

        @pl.when(turn == 1)
        def _():
            head_errors(lg[2])

        @pl.loop(0, num_layers - 1)
        def _(back):
            layer = num_layers - 1 - back
            backward_full(layer)
            for lower in range(num_layers - 1):
                @pl.when(jnp.logical_and(turn == 0, layer == lower + 1))
                def _():
                    dsend[lower] = dcat[...]
                    e_copies[0][lower].start()
                    e_copies[1][lower].start()

        backward_part(0, hs[0], dcat)

    pl.semaphore_signal(free_sem, inc=1, device_id=(mate,), device_id_type=MESH)

    @pl.loop(0, 2)
    def _(slot):
        for side in range(2):
            @pl.when(slot == side)
            def _():
                x_copies[side].wait_recv()
                l_copies[side].wait_recv()
        hs[0] = xg[slot]

        @pl.loop(0, num_layers)
        def _(layer):
            forward(layer, False)

        head_errors(lg[slot])
        backward_part(num_layers - 1, hs[num_layers - 1], dcat)

        @pl.when(slot == 1)
        def _():
            pl.semaphore_wait(free_sem, 1)
            p_copies[num_layers - 1].start()

        @pl.loop(0, num_layers - 2)
        def _(back):
            layer = num_layers - 2 - back
            for side in range(2):
                for lower in range(1, num_layers - 1):
                    @pl.when(jnp.logical_and(slot == side, layer == lower))
                    def _():
                        e_copies[side][lower].wait_recv()
            backward_part(layer, hs[layer], drecv.at[slot, layer])
            for lower in range(1, num_layers - 1):
                @pl.when(jnp.logical_and(slot == 1, layer == lower))
                def _():
                    p_copies[lower].start()

    @pl.loop(0, 2)
    def _(slot):
        for side in range(2):
            @pl.when(slot == side)
            def _():
                e_copies[side][0].wait_recv()
        backward_part(0, xg[slot], drecv.at[slot, 0])

    p_copies[0].start()
    for slot in range(3):
        x_copies[slot].wait_send()
        l_copies[slot].wait_send()
    for side in range(2):
        for lower in range(num_layers - 1):
            e_copies[side][lower].wait_send()

    sums = tuple(jnp.zeros((8, 128), F32) for _ in PAIRS)

    def fold(val):
        part = jnp.sum(val.reshape(-1, 8, val.shape[-1]), axis=0)
        out = part[:, :128]
        for piece in range(1, part.shape[-1] // 128):
            out = out + part[:, piece * 128:(piece + 1) * 128]
        return out

    for layer in range(num_layers - 1, -1, -1):
        p_copies[layer].wait_recv()

        @pl.loop(0, dim // rows48, init_carry=sums)
        def sums(block, carry):
            rows = pl.ds(pl.multiple_of(block * rows48, 8), rows48)
            grads = []
            for task in range(num_tasks):
                val = (acc[layer, task, core, rows] + pre[layer * num_tasks + task, rows]) * inv_tokens
                pre[layer * num_tasks + task, rows] = val
                grads.append(val)
            return tuple(old + fold(grads[t] * grads[s]) for old, (t, s) in zip(carry, PAIRS))

    for layer in range(num_layers):
        p_copies[layer].wait_send()
    tile_rows = lax.broadcasted_iota(jnp.int32, (8, 128), 0)
    my_tile = jnp.zeros((8, 128), F32)
    for row, val in enumerate(sums):
        my_tile = jnp.where(tile_rows == row, jnp.sum(val, axis=0, keepdims=True), my_tile)
    mtile[me] = my_tile
    m_copies = []
    for step in range(1, num_dev):
        m_copies.append(remote(mtile.at[me], mtile.at[me], ms_sem.at[step - 1], mr_sem.at[step - 1],
                               lax.rem(me + step, num_dev)))
        m_copies[-1].start()
    for step in range(1, num_dev):
        from_dev = lax.rem(me + num_dev - step, num_dev)
        remote(mtile.at[from_dev], mtile.at[from_dev], ms_sem.at[step - 1], mr_sem.at[step - 1],
               lax.rem(me + step, num_dev)).wait_recv()
    total = mtile[0]
    for dev in range(1, num_dev):
        total = total + mtile[dev]
    total = jnp.broadcast_to(jnp.sum(total, axis=1, keepdims=True), (8, 128))
    entry = {}
    for row, (t, s) in enumerate(PAIRS):
        val = jnp.broadcast_to(total[row:row + 1, :], (8, 128))
        entry[t, s] = val
        entry[s, t] = val
    tau = (entry[0, 0] + entry[1, 1] + entry[2, 2]) / num_tasks
    alpha = [jnp.full((8, 128), 1.0 / num_tasks, F32) for _ in range(num_tasks)]
    for step in range(EG_STEPS):
        pulls = [entry[t, 0] * alpha[0] + entry[t, 1] * alpha[1] + entry[t, 2] * alpha[2] for t in range(num_tasks)]
        alpha = [alpha[t] * jnp.exp(-pulls[t] / tau) for t in range(num_tasks)]
        norm = alpha[0] + alpha[1] + alpha[2]
        alpha = [a / norm for a in alpha]
    wts = [a[0:1, 0:1] for a in alpha]

    def mix(layer, rows):
        out = wts[0] * pre[layer * num_tasks, rows]
        for task in range(1, num_tasks):
            out = out + wts[task] * pre[layer * num_tasks + task, rows]
        return out

    for blk in range(CHIPS):
        rows = slice(blk * rows48, (blk + 1) * rows48)
        for layer in range(num_layers):
            acc[layer, 0, mcore, rows] = mix(layer, rows)
    g_copies = []
    for slot in range(3):
        g_src = acc.at[:, 0, mcore, pl.ds(pl.multiple_of(peer_chip[slot] * rows48, 8), rows48)]
        g_dst = acc.at[:, 1, mcore, pl.ds(slot * rows48, rows48)]
        g_copies.append(remote(g_src, g_dst, gs_sem.at[slot], gr_sem.at[slot], peers[slot]))
    for slot in (2, 0, 1):
        g_copies[slot].start()

    lanes = lax.broadcasted_iota(jnp.int32, (8, 128), 1)
    stat = jnp.zeros((8, 128), F32)
    for t in range(num_tasks):
        stat = jnp.where(jnp.logical_and(tile_rows == 0, lanes == t), alpha[t], stat)
        for s in range(num_tasks):
            stat = jnp.where(jnp.logical_and(tile_rows == 1 + t, lanes == s), entry[t, s], stat)
    stat_ref[...] = stat

    def put_rows(out_ref, layer, row0, row_tiles, col_tile, val):
        for piece in range(val.shape[1] // 128):
            start = row0 * row_tiles * num_layers + (col_tile + piece) * num_layers + layer
            out_ref[pl.ds(start, val.shape[0], stride=row_tiles * num_layers), :] = val[:, piece * 128:(piece + 1) * 128]

    @pl.loop(0, CHIPS)
    def _(block):
        rows = pl.ds(pl.multiple_of(half + block * rows48, 8), rows48)
        for layer in range(num_layers):
            put_rows(outd_ref, layer, block * rows48, dim // 128, 0, mix(layer, rows))

    own_rows = pl.ds(pl.multiple_of(chip * rows48, 8), rows48)
    for layer in range(num_layers):
        put_rows(outu_ref, layer, 0, ff // 128, chip * (ffq // 128), acc[layer, 0, mcore, own_rows])
    for slot in range(3):
        g_copies[slot].wait_recv()
        for layer in range(num_layers):
            put_rows(outu_ref, layer, 0, ff // 128, peer_chip[slot] * (ffq // 128),
                     acc[layer, 1, mcore, slot * rows48:(slot + 1) * rows48])
    for slot in range(3):
        g_copies[slot].wait_send()
    for copy in m_copies:
        copy.wait_send()


def solution(mesh):
    num_dev = mesh.shape['data']

    def local_step(x_local, lab_local, w_up, w_down, task_heads):
        num_layers, dim, ff = w_up.shape
        num_tasks = task_heads.shape[0]
        tok = x_local.shape[0]
        ffq = ff // CHIPS
        inv_tokens = 1.0 / (tok * num_dev)
        share = num_layers * dim * ff // num_dev // 128
        vmem = pl.BlockSpec(memory_space=pltpu.VMEM)
        hbm = pl.BlockSpec(memory_space=pl.ANY)

        def body(*refs):
            trunk_kernel(inv_tokens, *refs)

        dma = pltpu.SemaphoreType.DMA
        stat, out_up, out_down = pl.pallas_call(
            body,
            out_shape=(jax.ShapeDtypeStruct((8, 128), F32), jax.ShapeDtypeStruct((share, 128), F32),
                       jax.ShapeDtypeStruct((share, 128), F32)),
            in_specs=[vmem, vmem, hbm, hbm, vmem],
            out_specs=(vmem, vmem, vmem),
            scratch_shapes=[
                pltpu.VMEM((num_layers, dim, ff), BF16),
                pltpu.VMEM((num_layers, ff, dim), BF16),
                pltpu.VMEM((3, tok, dim), BF16),
                pltpu.VMEM((3, num_tasks, tok), jnp.int32),
                pltpu.VMEM((num_layers + 1, tok, dim), BF16),
                pltpu.VMEM(((num_layers - 1) * CHIPS, tok, ffq), F32),
                pltpu.VMEM((num_layers - 1, tok, ffq), BF16),
                pltpu.VMEM((tok, ffq), BF16),
                pltpu.VMEM((tok, num_tasks * dim), BF16),
                pltpu.VMEM((num_layers - 1, tok, num_tasks * dim), BF16),
                pltpu.VMEM((2, num_layers - 1, tok, num_tasks * dim), BF16),
                pltpu.VMEM((num_tasks, tok, ff), BF16),
                pltpu.VMEM((tok, num_tasks * ffq), BF16),
                pltpu.VMEM((num_layers, num_tasks, CORES, 2 * (dim // CORES), ffq), F32),
                pltpu.VMEM((num_dev, 8, 128), F32),
                dma((2, num_layers)), dma((3,)), dma((3,)), dma((3,)), dma((3,)),
                dma((2, num_layers - 1)), dma((2, num_layers - 1)), dma((num_layers,)), dma((num_layers,)),
                dma((num_dev - 1,)), dma((num_dev - 1,)), dma((3,)), dma((3,)), pltpu.SemaphoreType.REGULAR,
            ],
            compiler_params=pltpu.CompilerParams(
                collective_id=0, has_side_effects=True, vmem_limit_bytes=67043328),
        )(x_local, lab_local, w_up, w_down, jnp.transpose(task_heads, (0, 2, 1)))

        def unpack(packed):
            tiles = packed.reshape(share // num_layers, num_layers, 128)
            return jnp.transpose(tiles, (1, 0, 2)).reshape(num_layers, -1)

        return stat[0, :num_tasks], stat[1:1 + num_tasks, :num_tasks], unpack(out_up), unpack(out_down)

    return jax.shard_map(local_step, mesh=mesh, in_specs=(P('data', None), P(None, 'data'), P(), P(), P()),
                         out_specs=(P(), P(), P(None, 'data'), P(None, 'data')), check_vma=False)
```
